32 devices in a mesh: ex: 2 (over x), blk: 16 (over z, y, core).
Axes of the slice: x: 2, y: 2, z: 4, core: 2. Of those that a mesh axis runs over, the one named last changes fastest.
Arguments:
- activations: bfloat16 [256, 28672], P('blk', 'ex'), may hold values from -6 to 6
- out_grads: bfloat16 [256, 8192], P('ex', 'blk'), may hold values from -0.5 to 0.5
- basis_in: bfloat16 [28672, 28672], P('ex', 'blk'), may hold values from -0.03125 to 0.03125
- basis_out: bfloat16 [8192, 4096], P('blk', 'ex'), may hold values from -0.0625 to 0.0625
- example_ids: int32 [256], replicated, may hold values from 0 to 2, as said below
Outputs:
- correction: float32 [4096, 28672], P('ex', 'blk')
The draws below stay inside these ranges and needn't reach their ends.
Inputs may be any that keep to these rules, and one draw needn't show every extreme that they name: `example_ids`: example ids never fall along the tokens; every example 0 to 1 holds 1 to 192 tokens, and some example exactly 192; the id 2 marks padding tokens after the last example.
All inputs are finite; a program needn't handle non-finite values.
Results may differ from the reference program's by a relative error of at most 0.0029.
Values may be sent and summed in bfloat16 or wider, within the bound.
No kernel may reach another device: no remote copies, remote signals or barrier semaphores. Data moves between devices by JAX's collectives and lax.ppermute only.
A program may use at most 128 MiB of HBM per device.

```python
import jax
import jax.numpy as jnp
from jax import lax

F = 28672
OUT = 8192
OUTW = 4096
EXAMPLES = 2
TOKENS = 256
MOST = 192


def draw_example_ids(key, part):
    key_place = jax.random.fold_in(key, 11)
    key_lengths = jax.random.fold_in(key, 23)
    others = EXAMPLES - 1
    remain = TOKENS - MOST
    most_other = remain // others
    least_other = max(1, most_other // 2)
    other_lengths = jax.random.randint(key_lengths, (others,), least_other, most_other + 1).astype(jnp.int32)
    chosen = jax.random.randint(key_place, (), 0, EXAMPLES).astype(jnp.int32)
    position = jnp.arange(EXAMPLES, dtype=jnp.int32)
    before = other_lengths[jnp.clip(position, 0, others - 1)]
    after = other_lengths[jnp.clip(position - 1, 0, others - 1)]
    lengths = jnp.where(position < chosen, before, jnp.where(position == chosen, MOST, after)).astype(jnp.int32)
    ends = jnp.cumsum(lengths).astype(jnp.int32)
    tokens_at = jnp.arange(TOKENS, dtype=jnp.int32)
    return jnp.sum((ends[None, :] <= tokens_at[:, None]).astype(jnp.int32), axis=1).astype(jnp.int32)


def block_levels(stream_key, shape, cuts, smallest, largest):
    def one(axis_at, shards_of):
        steps = jax.random.uniform(jax.random.fold_in(jax.random.fold_in(stream_key, 6), axis_at), (shards_of,), jnp.float32, smallest / len(cuts), largest / len(cuts))
        return jnp.repeat(jnp.exp(steps), shape[axis_at] // shards_of).reshape((-1,) + (1,) * (len(shape) - axis_at - 1))

    factor_of = one(*cuts[0])
    for cut in cuts[1:]:
        factor_of = factor_of * one(*cut)
    return factor_of


def centred(rng, dims, width, most, pieces=(), kind=jnp.bfloat16):
    array = jax.random.normal(rng, dims, jnp.float32) * width
    if len(pieces) > 0:
        array = block_levels(rng, dims, pieces, -0.22, 0.18) * array
    return jnp.clip(array, min=-most, max=most).astype(kind)


def setup_inputs(seed: int = 0) -> dict:
    keys = jax.random.split(jax.random.key(seed), 6)
    activations = centred(keys[0], (TOKENS, F), 1.0, 6.0, ((0, 16), (1, 2)))
    out_grads = centred(keys[1], (TOKENS, OUT), 0.0625, 0.5, ((0, 2), (1, 16)))
    basis_in = centred(keys[2], (F, F), F ** -0.5, 0.03125, ((0, 2), (1, 16)))
    basis_out = centred(keys[3], (OUT, OUTW), OUT ** -0.5, 0.0625, ((0, 16), (1, 2)))
    example_ids = draw_example_ids(jax.random.fold_in(keys[5], 71), 0)
    return {"activations": activations, "out_grads": out_grads, "basis_in": basis_in, "basis_out": basis_out, "example_ids": example_ids}


def reference(activations, out_grads, basis_in, basis_out, example_ids):
    proj_in = jnp.dot(activations, basis_in, preferred_element_type=jnp.float32).astype(jnp.bfloat16)
    proj_out = jnp.dot(out_grads, basis_out, preferred_element_type=jnp.float32).astype(jnp.bfloat16)

    def add_example(example, running):
        offset = jnp.sum((example_ids < example).astype(jnp.int32))
        window_start = jnp.minimum(offset, TOKENS - MOST).astype(jnp.int32)
        window_ids = lax.dynamic_slice_in_dim(example_ids, window_start, MOST, 0)
        chosen = (window_ids == example).astype(proj_out.dtype)
        out_window = lax.dynamic_slice_in_dim(proj_out, window_start, MOST, 0) * chosen[:, None]
        in_window = lax.dynamic_slice_in_dim(proj_in, window_start, MOST, 0)
        example_grad = lax.dot_general(out_window, in_window, (((0,), (0,)), ((), ())), preferred_element_type=jnp.float32)
        return running + example_grad * example_grad

    running = lax.fori_loop(0, EXAMPLES, add_example, jnp.zeros((OUTW, F), jnp.float32))
    return running / EXAMPLES
```

```python
import functools

import jax
import jax.numpy as jnp
from jax import lax
from jax.experimental import pallas as pl
from jax.experimental.pallas import tpu as pltpu
from jax.sharding import PartitionSpec as P


LEN = 128
CHUNKS = 2
MIB = 2**20


def tile_of(width, most):
    return most if width % most == 0 else width


def project_out_body(where, *refs):
    *grads, basis, give, keep = refs
    for k, ref in enumerate(grads):
        term = lax.dot_general(
            basis[...], ref[...], (((0,), (1,)), ((), ())), preferred_element_type=jnp.float32
        )
        size = ref.shape[0]
        at = pl.ds(pl.multiple_of(where[1 + k] * size, size), size)

        @pl.when(pl.program_id(0) == 0)
        def _():
            give[:, at] = term

        @pl.when(pl.program_id(0) == 1)
        def _():
            keep[:, at] = term


def project_out(where, grads, basis):
    depth, width = basis.shape
    tokens = sum(g.shape[0] for g in grads)
    half = jax.ShapeDtypeStruct((width // 2, tokens), jnp.float32)
    fixed = lambda i, *_: (0, 0)
    return pl.pallas_call(
        project_out_body,
        grid_spec=pltpu.PrefetchScalarGridSpec(
            num_scalar_prefetch=1,
            grid=(2,),
            in_specs=[pl.BlockSpec(g.shape, fixed) for g in grads]
            + [pl.BlockSpec((depth, width // 2), lambda i, where: (0, (where[0] + 1 + i) % 2))],
            out_specs=[pl.BlockSpec(half.shape, fixed)] * 2,
        ),
        out_shape=[half, half],
        compiler_params=pltpu.CompilerParams(vmem_limit_bytes=12 * MIB),
        cost_estimate=pl.CostEstimate(flops=2 * depth * width * tokens, bytes_accessed=8 * MIB, transcendentals=0),
        name="project_out",
    )(where, *grads, basis)


def project_in_body(pieces, has_start, has_send, *refs):
    parts, refs = refs[:pieces], list(refs[pieces:])
    basis = refs.pop(0)
    start = refs.pop(0) if has_start else None
    packed = refs.pop()

    @pl.when(pl.program_id(0) == 0)
    def _():
        at = 0
        for ref in parts:
            packed[at:at + ref.shape[0], :] = ref[...]
            at += ref.shape[0]

    total = jnp.dot(packed[...], basis[...], preferred_element_type=jnp.float32)
    if has_start:
        total = start[...] + total
    refs[0][...] = total
    if has_send:
        refs[1][...] = total.astype(jnp.bfloat16)


def project_in(parts, basis, chunk, start, send, tile, first, last):
    depth = parts[0].shape[1]
    width = (last - first) * tile
    tokens = sum(p.shape[0] for p in parts)
    shapes = [jax.ShapeDtypeStruct((tokens, width), jnp.float32)]
    if send:
        shapes.append(jax.ShapeDtypeStruct((tokens, width), jnp.bfloat16))
    columns = pl.BlockSpec((tokens, tile), lambda i: (0, i))
    from_start = pl.BlockSpec((tokens, tile), lambda i: (0, first + i))
    return pl.pallas_call(
        functools.partial(project_in_body, len(parts), start is not None, send),
        grid=(width // tile,),
        in_specs=[pl.BlockSpec(p.shape, lambda i: (0, 0)) for p in parts]
        + [pl.BlockSpec((depth, tile), lambda i: (chunk, first + i))]
        + ([from_start] if start is not None else []),
        out_specs=[columns] * len(shapes),
        out_shape=shapes,
        scratch_shapes=[pltpu.VMEM((tokens, depth), jnp.bfloat16)],
        compiler_params=pltpu.CompilerParams(vmem_limit_bytes=28 * MIB),
        cost_estimate=pl.CostEstimate(
            flops=2 * tokens * depth * width, bytes_accessed=2 * depth * width, transcendentals=0
        ),
        name="project_in",
    )(*parts, basis, *([start] if start is not None else []))


def correct_body(examples, blocks, spans, order, rows, *refs):
    *found, ids, pieces, corr, proj, picked = refs
    size = proj.shape[0] // blocks
    count, step, _ = pieces.shape

    @pl.when(pl.program_id(0) == 0)
    def _():
        for t in range(blocks):
            at = pl.ds(t * size, size)
            to = pl.ds(pl.multiple_of(order[t] * size, size), size)
            begin = 0
            for span in range(spans):
                own, *others = found[span::spans]
                total = own[at, :]
                for ref in others:
                    total = total + ref[at, :].astype(jnp.float32)
                end = begin + own.shape[1]
                proj[to, begin:end] = total.astype(jnp.bfloat16)
                begin = end
        for m in range(count):
            piece = pieces[m]
            to = pl.ds(pl.multiple_of(rows[m] * step, step), step)
            for e in range(examples):
                picked[e, to, :] = jnp.where(ids[...] == e, piece, jnp.zeros_like(piece))

    tall = corr.shape[0]
    here = pl.ds(pl.multiple_of(pl.program_id(0) * tall, tall), tall)
    wide = tile_of(corr.shape[1], 256)
    for n in range(corr.shape[1] // wide):
        cols = slice(n * wide, (n + 1) * wide)
        running = None
        for e in range(examples):
            grad = jnp.dot(picked[e, here, :], proj[:, cols], preferred_element_type=jnp.float32)
            running = grad * grad if running is None else running + grad * grad
        corr[:, cols] = running / examples


def correction(order, rows, own, others, pieces, ids, examples, blocks):
    count, step, tokens = pieces.shape
    width = sum(o.shape[1] for o in own)
    whole = lambda m, *_: (0, 0)
    height = count * step
    tall = tile_of(height, 256)
    flops = 2 * examples * height * tokens * width
    return pl.pallas_call(
        functools.partial(correct_body, examples, blocks, len(own)),
        grid_spec=pltpu.PrefetchScalarGridSpec(
            num_scalar_prefetch=2,
            grid=(height // tall,),
            in_specs=[pl.BlockSpec(o.shape, whole) for o in (*own, *others)]
            + [pl.BlockSpec((1, tokens), whole), pl.BlockSpec(pieces.shape, lambda m, *_: (0, 0, 0))],
            out_specs=pl.BlockSpec((tall, width), lambda m, *_: (m, 0)),
            scratch_shapes=[
                pltpu.VMEM((tokens, width), jnp.bfloat16),
                pltpu.VMEM((examples, height, tokens), jnp.bfloat16),
            ],
        ),
        out_shape=jax.ShapeDtypeStruct((height, width), jnp.float32),
        compiler_params=pltpu.CompilerParams(vmem_limit_bytes=28 * MIB),
        cost_estimate=pl.CostEstimate(flops=flops, bytes_accessed=4 * height * width, transcendentals=0),
        name="correction",
    )(order, rows, *own, *others, ids, pieces)


def after(value, *earlier):
    return lax.optimization_barrier((value, *earlier))[0]


def local(parts, blocks, activations, out_grads, basis_in, basis_out, example_ids):
    line = blocks // 4
    me = lax.axis_index("blk")
    z, y, c = me // 4, (me // 2) % 2, me % 2

    def send(x, axis, size, to):
        return lax.ppermute(x, axis, [(i, to(i)) for i in range(size)])

    def core(x):
        return send(x, "blk", blocks, lambda i: i ^ 1)

    def side(x):
        return send(x, "blk", blocks, lambda i: i ^ 2)

    def shift(x, k):
        return send(x, "blk", blocks, lambda i: (i + 4 * k) % blocks)

    depth = activations.shape[1] // CHUNKS
    found = []
    for j in range(CHUNKS):
        own = activations[:, j * depth:(j + 1) * depth]
        rows = [own, side(own)]
        for k in range(1, line):
            far = shift(own, k)
            rows += [far, side(far)]
        found.append(rows)

    mine = lax.axis_index("ex")
    grads = [out_grads]
    for k in range(1, parts):
        grads.append(send(out_grads, "ex", parts, lambda i: (i + k) % parts))
    where = jnp.stack([c] + [(mine - k) % parts for k in range(parts)]).astype(jnp.int32)
    give, total = project_out(where, grads, basis_out)

    def picked(x, count, i):
        return lax.dynamic_index_in_dim(x.reshape(count, x.shape[0] // count, x.shape[1]), i, 0, keepdims=False)

    got = core(give)
    give = picked(total, 2, 1 - y) + picked(got, 2, 1 - y)
    total = picked(total, 2, y) + picked(got, 2, y)
    total = total + side(give)

    tile = tile_of(basis_in.shape[1], 256)
    tiles = basis_in.shape[1] // tile
    cuts = [0, (tiles + 1) // 2, tiles] if tiles > 1 else [0, tiles]
    partial_in = None
    for j in range(CHUNKS):
        rows = found[j]
        if partial_in is not None:
            rows = [after(r, partial_in) for r in rows]
        rows = rows + [core(r) for r in rows]
        if j < CHUNKS - 1:
            partial_in, = project_in(rows, basis_in, j, partial_in, False, tile, 0, tiles)
            if j == 0:
                total = after(total, partial_in)
                gifts = [shift(picked(total, line, (z + k) % line), k) for k in range(1, line)]
        else:
            sums = []
            for first, last in zip(cuts, cuts[1:]):
                sums.append(project_in(rows, basis_in, j, partial_in, parts == 2, tile, first, last))
    total = picked(after(total, sums[0][0]), line, z)
    for gift in gifts:
        total = total + gift
    piece = total.astype(jnp.bfloat16)
    out_line = jnp.stack([piece] + [shift(piece, k) for k in range(1, line)])
    out_side = jnp.concatenate([out_line, side(out_line)])
    proj_out = jnp.concatenate([out_side, core(out_side)])
    at = jnp.arange(blocks, dtype=jnp.int32)
    rows = (c ^ (at // (2 * line))) * (2 * line) + (y ^ (at // line % 2)) * line + (z - at % line) % line
    order = ((z - at % (2 * line) // 2) % line * 2 + (y ^ (at % 2))) * 2 + (c ^ (at // (2 * line)))

    if parts == 2:
        own = [s[0] for s in sums]
        others = [send(s[1], "ex", parts, lambda i: 1 - i) for s in sums]
    else:
        own = [lax.psum(s[0], "ex") for s in sums]
        others = []
    examples = example_ids.shape[0] // LEN
    return correction(order.astype(jnp.int32), rows.astype(jnp.int32), own, others, proj_out,
                      example_ids[None, :], examples, blocks)


def solution(mesh):
    parts, blocks = mesh.shape["ex"], mesh.shape["blk"]

    def body(*args):
        return local(parts, blocks, *args)

    return jax.shard_map(
        body,
        mesh=mesh,
        in_specs=(P("blk", "ex"), P("ex", "blk"), P("ex", "blk"), P("blk", "ex"), P()),
        out_specs=P("ex", "blk"),
        check_vma=False,
    )
```
